32 devices in a mesh: section: 4 (over z), tp: 4 (over y, core), dp: 2 (over x).
Axes of the slice: x: 2, y: 2, z: 4, core: 2. Of those that a mesh axis runs over, the one named last changes fastest.
Arguments:
- held: bfloat16 [4, 2, 128, 8192], P('section', 'dp', None, 'tp'), may hold values from -6 to 6
- incoming: bfloat16 [1, 2, 128, 8192], P(None, 'dp', None, 'tp'), may hold values from -6 to 6
- w_qkv: bfloat16 [4, 8192, 1536], P('section', None, 'tp'), may hold values from -0.0625 to 0.0625
- w_out: bfloat16 [4, 512, 8192], P('section', 'tp'), may hold values from -0.25 to 0.25
- norm_gain: bfloat16 [4, 8192], P('section'), may hold values from 0.099609375 to 1.8984375
Outputs:
- section_out: bfloat16 [2, 4, 2, 128, 8192], P(None, 'section', 'dp', None, 'tp')
- shadow_out: bfloat16 [2, 4, 2, 128, 8192], P(None, 'section', 'dp', None, 'tp')
The draws below stay inside these ranges and needn't reach their ends.
All inputs are finite; a program needn't handle non-finite values.
Results may differ from the reference program's by a relative error of at most 0.014.
Values may be sent and summed in bfloat16 or wider, within the bound.
No kernel may reach another device: no remote copies, remote signals or barrier semaphores. Data moves between devices by JAX's collectives and lax.ppermute only.
A program may use at most 128 MiB of HBM per device.

```python
import jax
import jax.numpy as jnp
from jax import lax

D = 8192
HD = 128
HEADS = 4
SEQ_LEN = 128
TICKS = 2
SECTIONS = 4
BATCH = 2


def block_levels(own_key, dims, pieces, least, high):
    factor_of = 1.0
    for position, blocks in pieces:
        steps = jax.random.uniform(jax.random.fold_in(jax.random.fold_in(own_key, 6), position), (blocks,), jnp.float32, least / len(pieces), high / len(pieces))
        factor_of = factor_of * jnp.repeat(jnp.exp(steps), dims[position] // blocks).reshape((-1,) + (1,) * (len(dims) - 1 - position))
    return factor_of


def normal_values(stream_key, dims, scale, bound, cuts=(), held_as=jnp.bfloat16):
    values = jax.random.normal(stream_key, dims, jnp.float32) * scale
    if len(cuts) > 0:
        values = block_levels(stream_key, dims, cuts, -0.22, 0.18) * values
    return jnp.clip(values, min=-bound, max=bound).astype(held_as)


def setup_inputs(seed: int = 0) -> dict:
    streams_of = jax.random.split(jax.random.key(seed), 6)
    return {
        "held": normal_values(streams_of[0], (SECTIONS, BATCH, SEQ_LEN, D), 1.0, 6.0, ((0, 4), (1, 2), (3, 4))),
        "incoming": normal_values(streams_of[1], (TICKS - 1, BATCH, SEQ_LEN, D), 1.0, 6.0, ((1, 2), (3, 4))),
        "w_qkv": normal_values(streams_of[2], (SECTIONS, D, HEADS * 3 * HD), D ** -0.5, 0.0625, ((0, 4), (2, 4))),
        "w_out": normal_values(streams_of[3], (SECTIONS, HEADS * HD, D), (HEADS * HD) ** -0.5, 0.25, ((0, 4), (1, 4))),
        "norm_gain": jnp.clip(1.0 + 0.18 * jax.random.normal(streams_of[4], (SECTIONS, D), jnp.float32), 0.099609375, 1.8984375).astype(jnp.bfloat16),
    }


EPS = 1e-05

def layer(source, w_proj, w_out, gain_row):
    batch, length, width = source.shape
    heads = w_proj.shape[1] // (3 * HD)
    values = source.astype(jnp.float32)
    scale = lax.rsqrt(lax.optimization_barrier(jnp.mean(values * values, axis=-1, keepdims=True)) + EPS)
    normed = (values * scale * gain_row.astype(jnp.float32)).astype(jnp.bfloat16)
    proj = jnp.dot(normed.reshape(batch * length, width), w_proj, preferred_element_type=jnp.float32)
    proj = proj.astype(jnp.bfloat16).reshape(batch, length, heads, 3, HD)
    query = proj[:, :, :, 0].astype(jnp.float32)
    key = proj[:, :, :, 1].astype(jnp.float32)
    value = proj[:, :, :, 2].astype(jnp.float32)
    scores = jnp.einsum('blhe,bmhe->bhlm', query, key) * HD ** (-0.5)
    causal = jnp.arange(length)[:, None] >= jnp.arange(length)[None, :]
    scores = jnp.where(causal[None, None], scores, -1e+30)
    weights = jax.nn.softmax(scores, axis=-1).astype(jnp.bfloat16)
    mixed = jnp.einsum('bhlm,bmhe->blhe', weights.astype(jnp.float32), value)
    mixed = mixed.astype(jnp.bfloat16).reshape(batch * length, heads * HD)
    delta = jnp.dot(mixed, w_out, preferred_element_type=jnp.float32).reshape(batch, length, width)
    return (values + delta).astype(jnp.bfloat16)

def reference(held, incoming, w_qkv, w_out, norm_gain):
    sections = held.shape[0]
    indices = jnp.arange(sections, dtype=jnp.int32)
    current = held
    outputs = []
    shadows = []
    for tick in range(TICKS):

        def own_layer(index, source=current):
            return layer(source[index], w_qkv[index], w_out[index], norm_gain[index])
        result = lax.map(own_layer, indices)

        def next_layer(index, source=result):
            after = ((index + 1) % sections).astype(jnp.int32)
            return layer(source[index], w_qkv[after], w_out[after], norm_gain[after])
        shadow = lax.map(next_layer, indices)
        outputs.append(result)
        shadows.append(shadow)
        if tick + 1 < TICKS:
            current = jnp.concatenate([incoming[tick][None], result[:-1]], axis=0)
    return (jnp.stack(outputs), jnp.stack(shadows))
```

```python
import functools

import jax
import jax.numpy as jnp
from jax import lax
from jax.experimental import pallas as pl
from jax.experimental.pallas import tpu as pltpu
from jax.sharding import PartitionSpec as P

HD = 128
TICKS = 2
EPS = 1e-05


def around(x, axis, by):
    length = lax.axis_size(axis)
    return lax.ppermute(x, axis, [(i, (i + by) % length) for i in range(length)])


def swapped(x, axis, bits):
    length = lax.axis_size(axis)
    return lax.ppermute(x, axis, [(i, i ^ bits) for i in range(length)])


def collected(block, axis):
    length = lax.axis_size(axis)
    pieces = {0: block}
    bit = length // 2
    while bit:
        pieces.update({k | bit: swapped(piece, axis, bit) for k, piece in list(pieces.items())})
        bit //= 2
    return [pieces[k] for k in range(length)]


def attend_body(place, *refs, count, sequences, width):
    pieces = refs[:count]
    w_ref, gain_ref, mixed_ref = refs[count : count + 3]
    x_buf, w_buf, x_sem, w_sem = refs[count + 3 :]
    mine = place[0]
    copies = []
    for k in range(count):
        rows = pl.ds((mine ^ k) * width, width)
        from_w = pltpu.make_async_copy(w_ref.at[rows], w_buf.at[k], w_sem.at[k])
        from_x = pltpu.make_async_copy(pieces[k], x_buf.at[k], x_sem.at[k])
        from_x.start()
        from_w.start()
        copies.append((from_x, from_w))
    total = None
    squares = None
    for k in range(count):
        copies[k][0].wait()
        values = x_buf[k].astype(jnp.float32)
        part = jnp.sum(values * values, axis=-1, keepdims=True)
        squares = part if squares is None else squares + part
        lifted = (values * gain_ref[mine ^ k].astype(jnp.float32)).astype(jnp.bfloat16)
        copies[k][1].wait()
        product = jnp.dot(lifted, w_buf[k], preferred_element_type=jnp.float32)
        total = product if total is None else total + product
    scale = lax.rsqrt(squares / (count * width) + EPS)
    proj = (total * scale).astype(jnp.bfloat16)
    heads = proj.shape[1] // (3 * HD)
    length = proj.shape[0] // sequences
    rows_at = lax.broadcasted_iota(jnp.int32, (length, length), 0)
    cols_at = lax.broadcasted_iota(jnp.int32, (length, length), 1)
    for b in range(sequences):
        for h in range(heads):
            part = proj[b * length : (b + 1) * length, h * 3 * HD : (h + 1) * 3 * HD]
            query, key, value = part[:, :HD], part[:, HD : 2 * HD], part[:, 2 * HD :]
            scores = lax.dot_general(
                query, key, (((1,), (1,)), ((), ())), preferred_element_type=jnp.float32
            ) * HD ** (-0.5)
            scores = jnp.where(rows_at >= cols_at, scores, -1e30)
            powers = jnp.exp(scores - jnp.max(scores, axis=-1, keepdims=True))
            weights = (powers / jnp.sum(powers, axis=-1, keepdims=True)).astype(jnp.bfloat16)
            mixed = jnp.dot(weights, value, preferred_element_type=jnp.float32)
            mixed_ref[b * length : (b + 1) * length, h * HD : (h + 1) * HD] = mixed.astype(
                jnp.bfloat16
            )


def attended(pieces, w_proj, gain_rows, place, sequences):
    count = len(pieces)
    rows, width = pieces[0].shape
    columns = w_proj.shape[1]
    anywhere = pl.BlockSpec(memory_space=pl.ANY)
    return pl.pallas_call(
        functools.partial(attend_body, count=count, sequences=sequences, width=width),
        out_shape=jax.ShapeDtypeStruct((rows, columns // 3), jnp.bfloat16),
        in_specs=[pl.BlockSpec(memory_space=pltpu.SMEM)]
        + [anywhere] * (count + 1)
        + [pl.BlockSpec(memory_space=pltpu.VMEM)],
        out_specs=pl.BlockSpec(memory_space=pltpu.VMEM),
        scratch_shapes=[
            pltpu.VMEM((count, rows, width), jnp.bfloat16),
            pltpu.VMEM((count, width, columns), jnp.bfloat16),
            pltpu.SemaphoreType.DMA((count,)),
            pltpu.SemaphoreType.DMA((count,)),
        ],
        name="attend",
    )(place, *pieces, w_proj, gain_rows)


def local(held, incoming, w_qkv, w_out, norm_gain):
    section = lax.axis_index("section")
    mine = lax.axis_index("tp")
    count = lax.axis_size("tp")
    _, sequences, length, width = held.shape
    rows = sequences * length
    w_proj = w_qkv[0]
    gain_rows = norm_gain.reshape(count, 1, width)
    place = mine.astype(jnp.int32).reshape(1)

    outs = []
    for k in range(count):
        wanted = lax.dynamic_slice_in_dim(w_out[0], (mine ^ k) * width, width, axis=1)
        outs.append(swapped(wanted, "tp", k) if k else wanted)
    out_columns = jnp.concatenate(outs, axis=0)

    def layer(block):
        mixed = attended(collected(block, "tp"), w_proj, gain_rows, place, sequences)
        mixed = jnp.concatenate(collected(mixed, "tp"), axis=1)
        added = jnp.dot(mixed, out_columns, preferred_element_type=jnp.float32)
        return (block.astype(jnp.float32) + added).astype(jnp.bfloat16)

    result = layer(held[0].reshape(rows, width))
    outputs = [result]
    shadows = []
    for tick in range(TICKS):
        layered = layer(around(result, "section", 1))
        shadows.append(around(layered, "section", -1))
        if tick + 1 < TICKS:
            fresh = layer(incoming[tick].reshape(rows, width))
            result = jnp.where(section == 0, fresh, layered)
            outputs.append(result)
    shape = (TICKS, 1, sequences, length, width)
    return (jnp.stack(outputs).reshape(shape), jnp.stack(shadows).reshape(shape))


def solution(mesh):
    placed = (
        P("section", "dp", None, "tp"),
        P(None, "dp", None, "tp"),
        P("section", None, "tp"),
        P("section", "tp", None),
        P("section", None),
    )
    out = P(None, "section", "dp", None, "tp")
    return jax.shard_map(
        local,
        mesh=mesh,
        in_specs=placed,
        out_specs=(out, out),
        check_vma=False,
    )
```
